32 devices in a mesh: gx: 4 (over x, core), gy: 2 (over y), gz: 4 (over z).
Axes of the slice: x: 2, y: 2, z: 4, core: 2. Of those that a mesh axis runs over, the one named last changes fastest.
Arguments:
- solution: float32 [16, 8, 16, 256], P(None, 'gx', 'gz', 'gy'), may hold values from -0.6 to 0.6
- residual: float32 [16, 8, 16, 256], P(None, 'gx', 'gz', 'gy'), may hold values from -6 to 6
- direction_prev: float32 [16, 8, 16, 256], P(None, 'gx', 'gz', 'gy'), may hold values from -0.3 to 0.3, as said below
- image_prev: float32 [16, 8, 16, 256], P(None, 'gx', 'gz', 'gy'), may hold values from -9 to 9, as said below
- gram_prev: float32 [16, 16], replicated, may hold values from -32768 to 32768, as said below
Outputs:
- solution_new: float32 [16, 8, 16, 256], P(None, 'gx', 'gz', 'gy')
- residual_new: float32 [16, 8, 16, 256], P(None, 'gx', 'gz', 'gy')
- direction: float32 [16, 8, 16, 256], P(None, 'gx', 'gz', 'gy')
The draws below stay inside these ranges and needn't reach their ends.
Inputs may be any that keep to these rules, and one draw needn't show every extreme that they name: direction_prev is a field of order 0.05. image_prev equals A direction_prev, computed in float32. gram_prev is symmetric and positive definite.
All inputs are finite; a program needn't handle non-finite values.
Results may differ from the reference program's by a relative error of at most 0.0001.
Values sent between devices are 32-bit elements; how exact they have to be, the bound alone decides.
A program may use at most 64 MiB of HBM per device.

```python
import jax
import jax.numpy as jnp
from jax import lax

RHS = 16
NX = 8
NZ = 16
NY = 256


def box_total(padded):
    total = padded[:, :-2] + padded[:, 1:-1] + padded[:, 2:]
    total = total[:, :, :-2] + total[:, :, 1:-1] + total[:, :, 2:]
    return total[:, :, :, :-2] + total[:, :, :, 1:-1] + total[:, :, :, 2:]


def shared_fields(key):
    base = jax.random.fold_in(key, 11)
    shape = (RHS, NX, NZ, NY)
    field = jnp.clip(0.04 * jax.random.normal(base, shape, jnp.float32), -0.24, 0.24)
    padded = jnp.pad(field, ((0, 0), (1, 1), (1, 1), (1, 1)))
    image = 27.0 * field - box_total(padded)
    return (field, image)


def draw_direction_prev(key, part):
    return shared_fields(key)[0]


def draw_image_prev(key, part):
    return shared_fields(key)[1]


def draw_gram_prev(key, part):
    base = jax.random.fold_in(key, 23)
    noise = jax.random.normal(base, (RHS, RHS), jnp.float32)
    matrix = jnp.eye(RHS, dtype=jnp.float32) + 0.05 * (noise + noise.T)
    return matrix * (NX * NY * NZ / 20.0)


def block_scale(key, extent, cuts, smallest, high):
    factor_of, own = 1.0, jax.random.fold_in(key, 6)
    for dim, parts in cuts:
        steps = jnp.exp(jax.random.uniform(jax.random.fold_in(own, dim), (parts,), jnp.float32, smallest / len(cuts), high / len(cuts)))
        factor_of = factor_of * jnp.repeat(steps, extent[dim] // parts).reshape([-1 if axis == dim else 1 for axis in range(len(extent))])
    return factor_of


def gaussian(key, extent, scale, limit, shards=(), kind=jnp.bfloat16):
    level = block_scale(key, extent, shards, -0.22, 0.18) if shards else 1.0
    drawn = jax.random.normal(key, extent, jnp.float32) * scale * level
    return jnp.minimum(jnp.maximum(drawn, -limit), limit).astype(kind)


def setup_inputs(seed: int = 0) -> dict:
    key_of = jax.random.split(jax.random.key(seed), 6)
    return {
        "solution": gaussian(key_of[0], (RHS, NX, NZ, NY), 0.1, 0.6, ((1, 4), (2, 4), (3, 2)), jnp.float32),
        "residual": gaussian(key_of[1], (RHS, NX, NZ, NY), 1.0, 6.0, ((1, 4), (2, 4), (3, 2)), jnp.float32),
        "direction_prev": draw_direction_prev(jax.random.fold_in(key_of[5], 71), 0),
        "image_prev": draw_image_prev(jax.random.fold_in(key_of[5], 71), 0),
        "gram_prev": draw_gram_prev(jax.random.fold_in(key_of[5], 71), 0),
    }


def pad_field(field):
    return jnp.pad(field, ((0, 0), (1, 1), (1, 1), (1, 1)))

def box_sum(padded):
    total = padded[:, :-2] + padded[:, 1:-1] + padded[:, 2:]
    total = total[:, :, :-2] + total[:, :, 1:-1] + total[:, :, 2:]
    return total[:, :, :, :-2] + total[:, :, :, 1:-1] + total[:, :, :, 2:]

def colors_of(shape):
    first = lax.broadcasted_iota(jnp.int32, shape, 1) % 2
    second = lax.broadcasted_iota(jnp.int32, shape, 2) % 2
    third = lax.broadcasted_iota(jnp.int32, shape, 3) % 2
    return 4 * first + 2 * second + third

def gram(left, right):
    return jnp.einsum('kxzy,lxzy->kl', left, right, precision=lax.Precision.HIGHEST)

def combine(field, mixing):
    return jnp.einsum('kxzy,kl->lxzy', field, mixing, precision=lax.Precision.HIGHEST)

def spd_solve(matrix, target):
    order = matrix.shape[0]
    sym = 0.5 * (matrix + matrix.T)
    lower = jnp.zeros_like(sym)
    for col in range(order):
        column = sym[col:, col] - lax.optimization_barrier(jnp.sum(lower[col:, :col] * lower[col, :col][None, :], axis=1))
        pivot = jnp.sqrt(column[0])
        lower = lower.at[col:, col].set(column / pivot)
    middle = jnp.zeros_like(target)
    for row in range(order):
        value = target[row] - lax.optimization_barrier(jnp.sum(lower[row, :row][:, None] * middle[:row], axis=0))
        middle = middle.at[row].set(value / lower[row, row])
    answer = jnp.zeros_like(target)
    for row in range(order - 1, -1, -1):
        value = middle[row] - lax.optimization_barrier(jnp.sum(lower[row + 1:, row][:, None] * answer[row + 1:], axis=0))
        answer = answer.at[row].set(value / lower[row, row])
    return answer

def reference(solution, residual, direction_prev, image_prev, gram_prev):
    colors = colors_of(residual.shape)
    smoothed = jnp.where(colors == 0, residual / 26.0, jnp.float32(0.0))
    for shade in list(range(1, 8)) + list(range(6, -1, -1)):
        boxed = box_sum(pad_field(smoothed))
        smoothed = jnp.where(colors == shade, (residual + boxed - smoothed) / 26.0, smoothed)
    image = 27.0 * smoothed - box_sum(pad_field(smoothed))
    gram_zr = gram(smoothed, residual)
    beta_mix = spd_solve(gram_prev, gram_zr)
    direction = smoothed + combine(direction_prev, beta_mix)
    image_new = image + combine(image_prev, beta_mix)
    curvature = gram(direction, image_new)
    alpha_step = spd_solve(curvature, gram_zr)
    solution_new = solution + combine(direction, alpha_step)
    residual_new = residual - combine(image_new, alpha_step)
    return (solution_new, residual_new, direction)
```

```python
import functools

import jax
import jax.numpy as jnp
from jax import lax
from jax.experimental import pallas as pl
from jax.experimental.pallas import tpu as pltpu
from jax.sharding import PartitionSpec as P


def with_halo(value, sides, width):
    for axis, dim in sides:
        devices, length = (lax.axis_size(axis), value.shape[dim])
        up = [(i, (i + 1) % devices) for i in range(devices - 1)]
        down = [(j, i) for i, j in up]
        last = lax.slice_in_dim(value, length - width, length, axis=dim)
        first = lax.slice_in_dim(value, 0, width, axis=dim)
        before = lax.ppermute(last, axis, up)
        after = lax.ppermute(first, axis, down)
        value = jnp.concatenate([before, value, after], axis=dim)
    return value


def box_sum(padded):
    total = padded[:, :-2] + padded[:, 1:-1] + padded[:, 2:]
    total = total[:, :, :-2] + total[:, :, 1:-1] + total[:, :, 2:]
    return total[:, :, :, :-2] + total[:, :, :, 1:-1] + total[:, :, :, 2:]


def colors_of(shape):
    first = lax.broadcasted_iota(jnp.int32, shape, 1) % 2
    second = lax.broadcasted_iota(jnp.int32, shape, 2) % 2
    third = lax.broadcasted_iota(jnp.int32, shape, 3) % 2
    return 4 * first + 2 * second + third


def local_gram(left, right):
    return jnp.einsum("kxzy,lxzy->kl", left, right, precision=lax.Precision.HIGHEST)


def combine(field, mixing):
    return jnp.einsum("kxzy,kl->lxzy", field, mixing, precision=lax.Precision.HIGHEST)


def small_dot(left, right):
    return jnp.dot(left, right, precision=lax.Precision.HIGHEST)


def spd_solve(matrix, target):
    order = matrix.shape[0]
    sym = 0.5 * (matrix + matrix.T)
    lower = jnp.zeros_like(sym)
    for col in range(order):
        column = sym[col:, col] - jnp.sum(lower[col:, :col] * lower[col, :col][None, :], axis=1)
        pivot = jnp.sqrt(column[0])
        lower = lower.at[col:, col].set(column / pivot)
    middle = jnp.zeros_like(target)
    for row in range(order):
        value = target[row] - jnp.sum(lower[row, :row][:, None] * middle[:row], axis=0)
        middle = middle.at[row].set(value / lower[row, row])
    answer = jnp.zeros_like(target)
    for row in range(order - 1, -1, -1):
        value = middle[row] - jnp.sum(lower[row + 1 :, row][:, None] * answer[row + 1 :], axis=0)
        answer = answer.at[row].set(value / lower[row, row])
    return answer


def sweep_box(field):
    padded = with_halo(field, (("gx", 1), ("gy", 3), ("gz", 2)), 1)
    return box_sum(padded)


def body(solution, residual, direction_prev, image_prev, gram_prev):
    colors = colors_of(residual.shape)
    smoothed = jnp.where(colors == 0, residual / 26.0, jnp.float32(0.0))
    for shade in list(range(1, 8)) + list(range(6, -1, -1)):
        boxed = sweep_box(smoothed)
        smoothed = jnp.where(colors == shade, (residual + boxed - smoothed) / 26.0, smoothed)
    padded = with_halo(smoothed, (("gx", 1), ("gy", 3), ("gz", 2)), 1)
    image = 27.0 * smoothed - box_sum(padded)
    sums = (
        local_gram(smoothed, residual),
        local_gram(smoothed, image),
        local_gram(smoothed, image_prev),
        local_gram(direction_prev, image),
        local_gram(direction_prev, image_prev),
    )
    gram_zr, gram_zw, gram_zq, gram_pw, gram_pq = lax.psum(
        (sums[0], sums[1], sums[2], sums[3], sums[4]), ("gx", "gy", "gz")
    )
    beta_mix = spd_solve(gram_prev, gram_zr)
    direction = smoothed + combine(direction_prev, beta_mix)
    image_new = image + combine(image_prev, beta_mix)
    curvature = gram_zw + small_dot(gram_zq, beta_mix) + small_dot(beta_mix.T, gram_pw)
    curvature = curvature + small_dot(small_dot(beta_mix.T, gram_pq), beta_mix)
    alpha_step = spd_solve(curvature, gram_zr)
    solution_new = solution + combine(direction, alpha_step)
    residual_new = residual - combine(image_new, alpha_step)
    return (solution_new, residual_new, direction)


MESH = pl.DeviceIdType.MESH
HIGHEST = lax.Precision.HIGHEST


def dot(left, right):
    return jnp.dot(left, right, precision=HIGHEST, preferred_element_type=jnp.float32)


def dot_nt(left, right):
    return lax.dot_general(
        left, right, (((1,), (1,)), ((), ())), precision=HIGHEST, preferred_element_type=jnp.float32
    )


def eliminate(matrix, target):
    matrix = 0.5 * (matrix + matrix.T)
    order = matrix.shape[0]
    rows = lax.broadcasted_iota(jnp.int32, matrix.shape, 0)
    for c in range(order):
        column = jnp.broadcast_to(matrix[:, c : c + 1], matrix.shape)
        scale = 1.0 / column[c : c + 1, :]
        mrow = matrix[c : c + 1, :] * scale
        trow = target[c : c + 1, :] * scale
        here = rows == c
        target = jnp.where(here, trow, target - column * trow)
        if c < order - 1:
            matrix = jnp.where(here, mrow, matrix - column * mrow)
    return target


def smooth(res, ngx, ngz):
    lx, lz = len(res), len(res[0])
    count, ny = res[0][0].shape
    row = lax.broadcasted_iota(jnp.int32, (count, ny), 0)
    lane = lax.broadcasted_iota(jnp.int32, (count, ny), 1)
    even = lane % 2 == 0
    edges = {
        "xp": (row < ngz, ngz, 0),
        "xn": (row >= count - ngz, count - ngz, 0),
        "zp": (row % ngz == 0, 1, 0),
        "zn": (row % ngz == ngz - 1, count - 1, 0),
        "yp": (lane == 0, 1, 1),
        "yn": (lane == ny - 1, ny - 1, 1),
    }
    zero = jnp.zeros((count, ny), jnp.float32)
    memo = {}

    def moved(value, kind):
        if value is None:
            return None
        key = (kind, id(value))
        if key not in memo:
            edge, amount, axis = edges[kind]
            memo[key] = (value, jnp.where(edge, zero, pltpu.roll(value, amount, axis)))
        return memo[key][1]

    def add(*values):
        total = None
        for value in values:
            if value is not None:
                total = value if total is None else total + value
        return total

    state = {(x, z): None for x in range(lx) for z in range(lz)}

    def z_pair(x, z):
        before = state[x, z - 1] if z > 0 else moved(state[x, lz - 1], "zp")
        after = state[x, z + 1] if z < lz - 1 else moved(state[x, 0], "zn")
        return add(before, after)

    def neighbours(x, z):
        def line(other):
            return add(state[other, z], z_pair(other, z))

        before = line(x - 1) if x > 0 else moved_line(lx - 1, z, "xp")
        after = line(x + 1) if x < lx - 1 else moved_line(0, z, "xn")
        return add(z_pair(x, z), before, after)

    def moved_line(x, z, kind):
        return moved(add(state[x, z], z_pair(x, z)), kind)

    def y_pair(value):
        return moved(value, "yp") + moved(value, "yn")

    third = jnp.float32(1.0 / 26.0)
    plan = [(0, 0, (0, 1)), (0, 1, (0, 1)), (1, 0, (0, 1)), (1, 1, (0, 1, 0)), (1, 0, (1, 0)), (0, 1, (1, 0)), (0, 0, (1, 0))]
    for xp, zp, shades in plan:
        fresh = {}
        for x in range(xp, lx, 2):
            for z in range(zp, lz, 2):
                near = neighbours(x, z)
                base = res[x][z] if near is None else res[x][z] + (near + y_pair(near))
                value = state[x, z]
                for shade in shades:
                    total = base if value is None else base + y_pair(value)
                    chosen = even if shade == 0 else jnp.logical_not(even)
                    value = jnp.where(chosen, total * third, zero if value is None else value)
                fresh[x, z] = value
        state.update(fresh)
    image = {}
    for x in range(lx):
        for z in range(lz):
            box = add(state[x, z], neighbours(x, z))
            image[x, z] = 27.0 * state[x, z] - (box + y_pair(box))
    return state, image


def kernel(
    sizes, sol_in, res_in, dir_in, img_in, gram_in, sol_out, res_out, dir_out,
    sol, res, prev, prev_img, gram, outs, land, done, back, part, parts,
    local_sem, send_a, send_b, send_c, recv_sem,
):
    ngx, ngy, ngz, n, lx, lz, width = sizes
    s = lx * lz
    gx, gy, gz = lax.axis_index("gx"), lax.axis_index("gy"), lax.axis_index("gz")
    column = gx * ngz + gz
    place = gy * n + column
    everyone = n * ngy

    loads = [
        pltpu.make_async_copy(a, b, local_sem.at[i])
        for i, (a, b) in enumerate(((res_in, res), (gram_in, gram), (dir_in, prev), (img_in, prev_img), (sol_in, sol)))
    ]
    for load in loads:
        load.start()

    def peer(offset):
        other = lax.rem(place + offset, everyone)
        oy, oc = other // n, lax.rem(other, n)
        return oc, {"gx": oc // ngz, "gy": oy, "gz": lax.rem(oc, ngz)}

    barrier = pltpu.get_barrier_semaphore()
    for offset in range(1, everyone):
        pl.semaphore_signal(barrier, inc=1, device_id=peer(offset)[1], device_id_type=MESH)
    loads[0].wait()
    pl.semaphore_wait(barrier, everyone - 1)

    sent = []
    mine = land.at[pl.ds(place * s, s), :]
    for offset in range(1, everyone):
        oc, where = peer(offset)
        copy = pltpu.make_async_remote_copy(
            src_ref=res.at[pl.ds(oc * s, s), :], dst_ref=mine,
            send_sem=send_a.at[offset], recv_sem=recv_sem.at[0], device_id=where, device_id_type=MESH,
        )
        copy.start()
        sent.append(copy)
    pltpu.make_async_copy(res.at[pl.ds(column * s, s), :], mine, recv_sem.at[0]).start()

    def flat(ref, first, stride):
        return jnp.concatenate([ref[pl.ds(first + i, n, stride=stride), :] for i in range(s)], axis=1)

    for load in loads[1:4]:
        load.wait()
    eye = (lax.broadcasted_iota(jnp.int32, (n, n), 0) == lax.broadcasted_iota(jnp.int32, (n, n), 1)).astype(jnp.float32)
    inverse = eliminate(gram[...], eye)
    p, q, r = flat(prev, 0, s), flat(prev_img, 0, s), flat(res, 0, s)
    gram_pq = dot_nt(p, q)

    pltpu.make_async_copy(land, land, recv_sem.at[0]).wait()
    field = [
        [
            jnp.concatenate(
                [land[pl.ds(y * n * s + x * lz + z, n, stride=s), :] for y in range(ngy)], axis=1
            )
            for z in range(lz)
        ]
        for x in range(lx)
    ]
    state, image = smooth(field, ngx, ngz)
    for x in range(lx):
        for z in range(lz):
            for y in range(ngy):
                first = y * n * 2 * s + x * lz + z
                cut = slice(y * width, (y + 1) * width)
                done[pl.ds(first, n, stride=2 * s), :] = state[x, z][:, cut]
                done[pl.ds(first + s, n, stride=2 * s), :] = image[x, z][:, cut]
    mine = back.at[pl.ds(column * 2 * s, 2 * s), :]
    for offset in range(1, n):
        oc = lax.rem(column + offset, n)
        copy = pltpu.make_async_remote_copy(
            src_ref=done.at[pl.ds((gy * n + oc) * 2 * s, 2 * s), :], dst_ref=mine,
            send_sem=send_b.at[offset], recv_sem=recv_sem.at[1],
            device_id={"gx": oc // ngz, "gy": gy, "gz": lax.rem(oc, ngz)}, device_id_type=MESH,
        )
        copy.start()
        sent.append(copy)
    pltpu.make_async_copy(done.at[pl.ds(place * 2 * s, 2 * s), :], mine, recv_sem.at[1]).start()
    pltpu.make_async_copy(back, back, recv_sem.at[1]).wait()

    zf, wf = flat(back, 0, 2 * s), flat(back, s, 2 * s)
    sums = dot_nt(zf, jnp.concatenate([r, wf, q], axis=0))
    sums = jnp.concatenate([sums, gram_pq], axis=1)
    half = n // 2
    part[...] = jnp.concatenate([sums[:half], sums[half:]], axis=1)
    mine = parts.at[pl.ds(place * half, half), :]
    for offset in range(1, everyone):
        copy = pltpu.make_async_remote_copy(
            src_ref=part, dst_ref=mine,
            send_sem=send_c.at[offset], recv_sem=recv_sem.at[2], device_id=peer(offset)[1], device_id_type=MESH,
        )
        copy.start()
        sent.append(copy)
    pltpu.make_async_copy(part, mine, recv_sem.at[2]).start()
    pltpu.make_async_copy(parts, parts, recv_sem.at[2]).wait()

    level = [parts[i * half : (i + 1) * half, :] for i in range(everyone)]
    while len(level) > 1:
        level = [sum(level[i + 1 : i + 2], level[i]) for i in range(0, len(level), 2)]
    total = level[0]
    total = jnp.concatenate([total[:, : 4 * n], total[:, 4 * n :]], axis=0)
    gram_zr, gram_zw, gram_zq, gram_pq = (total[:, i * n : (i + 1) * n] for i in range(4))

    beta = dot(inverse, gram_zr)
    cross = dot(jnp.concatenate([gram_zq, gram_pq], axis=0), beta)
    beta_t = beta.T
    curvature = gram_zw + cross[:n] + cross[:n].T + dot(beta_t, cross[n:])
    mixed = dot(beta_t, jnp.concatenate([p, q], axis=1))
    direction = zf + mixed[:, : s * width]
    image_new = wf + mixed[:, s * width :]
    alpha = eliminate(curvature, gram_zr)
    step = dot(alpha.T, jnp.concatenate([direction, image_new], axis=1))
    loads[4].wait()
    for i in range(s):
        rows = pl.ds(i, n, stride=s)
        cut = slice(i * width, (i + 1) * width)
        outs[2, rows, :] = direction[:, cut]
        outs[0, rows, :] = sol[rows, :] + step[:, cut]
        outs[1, rows, :] = res[rows, :] - step[:, s * width + i * width : s * width + (i + 1) * width]
    stores = [
        pltpu.make_async_copy(outs.at[i], out, local_sem.at[i]) for i, out in enumerate((sol_out, res_out, dir_out))
    ]
    for store in stores:
        store.start()
    for copy in sent:
        copy.wait_send()
    for store in stores:
        store.wait()


def whole_body(sizes, solution, residual, direction_prev, image_prev, gram_prev):
    ngx, ngy, ngz, n, lx, lz, width = sizes
    s, everyone = lx * lz, n * ngy
    rows = n * s
    shape = residual.shape
    field = jax.ShapeDtypeStruct((rows, width), jnp.float32)
    outs = pl.pallas_call(
        functools.partial(kernel, sizes),
        out_shape=(field, field, field),
        in_specs=[pl.BlockSpec(memory_space=pl.ANY)] * 5,
        out_specs=[pl.BlockSpec(memory_space=pl.ANY)] * 3,
        scratch_shapes=[pltpu.VMEM((rows, width), jnp.float32)] * 4
        + [
            pltpu.VMEM((n, n), jnp.float32),
            pltpu.VMEM((3, rows, width), jnp.float32),
            pltpu.VMEM((everyone * s, width), jnp.float32),
            pltpu.VMEM((everyone * 2 * s, width), jnp.float32),
            pltpu.VMEM((n * 2 * s, width), jnp.float32),
            pltpu.VMEM((n // 2, 8 * n), jnp.float32),
            pltpu.VMEM((everyone * (n // 2), 8 * n), jnp.float32),
            pltpu.SemaphoreType.DMA((5,)),
            pltpu.SemaphoreType.DMA((everyone,)),
            pltpu.SemaphoreType.DMA((n,)),
            pltpu.SemaphoreType.DMA((everyone,)),
            pltpu.SemaphoreType.DMA((3,)),
        ],
        compiler_params=pltpu.CompilerParams(collective_id=0, has_side_effects=True),
    )(*(a.reshape(rows, width) for a in (solution, residual, direction_prev, image_prev)), gram_prev)
    return tuple(a.reshape(shape) for a in outs)


def pick_body(mesh, solution, residual, direction_prev, image_prev, gram_prev):
    ngx, ngy, ngz = (mesh.shape[axis] for axis in ("gx", "gy", "gz"))
    n, lx, lz, width = residual.shape
    fits = n == ngx * ngz and lx % 2 == 0 and lz % 2 == 0 and (lx * lz) % 8 == 0
    fits = fits and width % 128 == 0 and n % 16 == 0
    args = (solution, residual, direction_prev, image_prev, gram_prev)
    if fits:
        return whole_body((ngx, ngy, ngz, n, lx, lz, width), *args)
    return body(*args)


def solution(mesh):
    in_specs = (
        P(None, "gx", "gz", "gy"),
        P(None, "gx", "gz", "gy"),
        P(None, "gx", "gz", "gy"),
        P(None, "gx", "gz", "gy"),
        P(),
    )
    out_specs = (P(None, "gx", "gz", "gy"), P(None, "gx", "gz", "gy"), P(None, "gx", "gz", "gy"))
    return jax.shard_map(functools.partial(pick_body, mesh), mesh=mesh, in_specs=in_specs, out_specs=out_specs, check_vma=False)
```

```python
import functools

import jax
import jax.numpy as jnp
from jax import lax
from jax.experimental import pallas as pl
from jax.experimental.pallas import tpu as pltpu
from jax.sharding import PartitionSpec as P


def with_halo(value, sides, width):
    for axis, dim in sides:
        devices, length = (lax.axis_size(axis), value.shape[dim])
        up = [(i, (i + 1) % devices) for i in range(devices - 1)]
        down = [(j, i) for i, j in up]
        last = lax.slice_in_dim(value, length - width, length, axis=dim)
        first = lax.slice_in_dim(value, 0, width, axis=dim)
        before = lax.ppermute(last, axis, up)
        after = lax.ppermute(first, axis, down)
        value = jnp.concatenate([before, value, after], axis=dim)
    return value


def box_sum(padded):
    total = padded[:, :-2] + padded[:, 1:-1] + padded[:, 2:]
    total = total[:, :, :-2] + total[:, :, 1:-1] + total[:, :, 2:]
    return total[:, :, :, :-2] + total[:, :, :, 1:-1] + total[:, :, :, 2:]


def colors_of(shape):
    first = lax.broadcasted_iota(jnp.int32, shape, 1) % 2
    second = lax.broadcasted_iota(jnp.int32, shape, 2) % 2
    third = lax.broadcasted_iota(jnp.int32, shape, 3) % 2
    return 4 * first + 2 * second + third


def local_gram(left, right):
    return jnp.einsum("kxzy,lxzy->kl", left, right, precision=lax.Precision.HIGHEST)


def combine(field, mixing):
    return jnp.einsum("kxzy,kl->lxzy", field, mixing, precision=lax.Precision.HIGHEST)


def small_dot(left, right):
    return jnp.dot(left, right, precision=lax.Precision.HIGHEST)


def spd_solve(matrix, target):
    order = matrix.shape[0]
    sym = 0.5 * (matrix + matrix.T)
    lower = jnp.zeros_like(sym)
    for col in range(order):
        column = sym[col:, col] - jnp.sum(lower[col:, :col] * lower[col, :col][None, :], axis=1)
        pivot = jnp.sqrt(column[0])
        lower = lower.at[col:, col].set(column / pivot)
    middle = jnp.zeros_like(target)
    for row in range(order):
        value = target[row] - jnp.sum(lower[row, :row][:, None] * middle[:row], axis=0)
        middle = middle.at[row].set(value / lower[row, row])
    answer = jnp.zeros_like(target)
    for row in range(order - 1, -1, -1):
        value = middle[row] - jnp.sum(lower[row + 1 :, row][:, None] * answer[row + 1 :], axis=0)
        answer = answer.at[row].set(value / lower[row, row])
    return answer


def sweep_box(field):
    padded = with_halo(field, (("gx", 1), ("gy", 3), ("gz", 2)), 1)
    return box_sum(padded)


def body(solution, residual, direction_prev, image_prev, gram_prev):
    colors = colors_of(residual.shape)
    smoothed = jnp.where(colors == 0, residual / 26.0, jnp.float32(0.0))
    for shade in list(range(1, 8)) + list(range(6, -1, -1)):
        boxed = sweep_box(smoothed)
        smoothed = jnp.where(colors == shade, (residual + boxed - smoothed) / 26.0, smoothed)
    padded = with_halo(smoothed, (("gx", 1), ("gy", 3), ("gz", 2)), 1)
    image = 27.0 * smoothed - box_sum(padded)
    sums = (
        local_gram(smoothed, residual),
        local_gram(smoothed, image),
        local_gram(smoothed, image_prev),
        local_gram(direction_prev, image),
        local_gram(direction_prev, image_prev),
    )
    gram_zr, gram_zw, gram_zq, gram_pw, gram_pq = lax.psum(
        (sums[0], sums[1], sums[2], sums[3], sums[4]), ("gx", "gy", "gz")
    )
    beta_mix = spd_solve(gram_prev, gram_zr)
    direction = smoothed + combine(direction_prev, beta_mix)
    image_new = image + combine(image_prev, beta_mix)
    curvature = gram_zw + small_dot(gram_zq, beta_mix) + small_dot(beta_mix.T, gram_pw)
    curvature = curvature + small_dot(small_dot(beta_mix.T, gram_pq), beta_mix)
    alpha_step = spd_solve(curvature, gram_zr)
    solution_new = solution + combine(direction, alpha_step)
    residual_new = residual - combine(image_new, alpha_step)
    return (solution_new, residual_new, direction)


MESH = pl.DeviceIdType.MESH
HIGHEST = lax.Precision.HIGHEST


def dot(left, right):
    return jnp.dot(left, right, precision=HIGHEST, preferred_element_type=jnp.float32)


def dot_nt(left, right):
    return lax.dot_general(
        left, right, (((1,), (1,)), ((), ())), precision=HIGHEST, preferred_element_type=jnp.float32
    )


def eliminate(matrix, target):
    matrix = 0.5 * (matrix + matrix.T)
    order = matrix.shape[0]
    rows = lax.broadcasted_iota(jnp.int32, matrix.shape, 0)
    for c in range(order):
        column = jnp.broadcast_to(matrix[:, c : c + 1], matrix.shape)
        scale = 1.0 / column[c : c + 1, :]
        mrow = matrix[c : c + 1, :] * scale
        trow = target[c : c + 1, :] * scale
        here = rows == c
        target = jnp.where(here, trow, target - column * trow)
        if c < order - 1:
            matrix = jnp.where(here, mrow, matrix - column * mrow)
    return target


def smooth(res, ngx, ngz):
    lx, lz = len(res), len(res[0])
    count, ny = res[0][0].shape
    row = lax.broadcasted_iota(jnp.int32, (count, ny), 0)
    lane = lax.broadcasted_iota(jnp.int32, (count, ny), 1)
    even = lane % 2 == 0
    edges = {
        "xp": (row < ngz, ngz, 0),
        "xn": (row >= count - ngz, count - ngz, 0),
        "zp": (row % ngz == 0, 1, 0),
        "zn": (row % ngz == ngz - 1, count - 1, 0),
        "yp": (lane == 0, 1, 1),
        "yn": (lane == ny - 1, ny - 1, 1),
    }
    zero = jnp.zeros((count, ny), jnp.float32)
    memo = {}

    def moved(value, kind):
        if value is None:
            return None
        key = (kind, id(value))
        if key not in memo:
            edge, amount, axis = edges[kind]
            memo[key] = (value, jnp.where(edge, zero, pltpu.roll(value, amount, axis)))
        return memo[key][1]

    def add(*values):
        total = None
        for value in values:
            if value is not None:
                total = value if total is None else total + value
        return total

    state = {(x, z): None for x in range(lx) for z in range(lz)}

    def z_pair(x, z):
        before = state[x, z - 1] if z > 0 else moved(state[x, lz - 1], "zp")
        after = state[x, z + 1] if z < lz - 1 else moved(state[x, 0], "zn")
        return add(before, after)

    def neighbours(x, z):
        def line(other):
            return add(state[other, z], z_pair(other, z))

        before = line(x - 1) if x > 0 else moved_line(lx - 1, z, "xp")
        after = line(x + 1) if x < lx - 1 else moved_line(0, z, "xn")
        return add(z_pair(x, z), before, after)

    def moved_line(x, z, kind):
        return moved(add(state[x, z], z_pair(x, z)), kind)

    def y_pair(value):
        return moved(value, "yp") + moved(value, "yn")

    third = jnp.float32(1.0 / 26.0)
    plan = [(0, 0, (0, 1)), (0, 1, (0, 1)), (1, 0, (0, 1)), (1, 1, (0, 1, 0)), (1, 0, (1, 0)), (0, 1, (1, 0)), (0, 0, (1, 0))]
    for xp, zp, shades in plan:
        fresh = {}
        for x in range(xp, lx, 2):
            for z in range(zp, lz, 2):
                near = neighbours(x, z)
                base = res[x][z] if near is None else res[x][z] + (near + y_pair(near))
                value = state[x, z]
                for shade in shades:
                    total = base if value is None else base + y_pair(value)
                    chosen = even if shade == 0 else jnp.logical_not(even)
                    value = jnp.where(chosen, total * third, zero if value is None else value)
                fresh[x, z] = value
        state.update(fresh)
    image = {}
    for x in range(lx):
        for z in range(lz):
            box = add(state[x, z], neighbours(x, z))
            image[x, z] = 27.0 * state[x, z] - (box + y_pair(box))
    return state, image


def kernel(
    sizes, res_in, dir_in, img_in, gram_in, back_out, small_out,
    res, prev, prev_img, gram, small, land, done, back, part, parts,
    local_sem, send_a, send_b, send_c, recv_sem,
):
    ngx, ngy, ngz, n, lx, lz, width = sizes
    s = lx * lz
    gx, gy, gz = lax.axis_index("gx"), lax.axis_index("gy"), lax.axis_index("gz")
    column = gx * ngz + gz
    place = gy * n + column
    everyone = n * ngy

    loads = [
        pltpu.make_async_copy(a, b, local_sem.at[i])
        for i, (a, b) in enumerate(((res_in, res), (gram_in, gram), (dir_in, prev), (img_in, prev_img)))
    ]
    for load in loads:
        load.start()

    ways = sorted(
        ((dx, dy, dz) for dx in range(ngx) for dy in range(ngy) for dz in range(ngz)),
        key=lambda way: (-min(way[2], ngz - way[2]), -min(way[0], ngx - way[0]), -way[1]),
    )[:-1]

    def peer(offset):
        dx, dy, dz = ways[offset - 1]
        ox, oy, oz = lax.rem(gx + dx, ngx), lax.rem(gy + dy, ngy), lax.rem(gz + dz, ngz)
        return ox * ngz + oz, {"gx": ox, "gy": oy, "gz": oz}

    barrier = pltpu.get_barrier_semaphore()
    for offset in range(1, everyone):
        pl.semaphore_signal(barrier, inc=1, device_id=peer(offset)[1], device_id_type=MESH)
    loads[0].wait()
    pl.semaphore_wait(barrier, everyone - 1)

    sent = []
    mine = land.at[pl.ds(place * s, s), :]
    for offset in range(1, everyone):
        oc, where = peer(offset)
        copy = pltpu.make_async_remote_copy(
            src_ref=res.at[pl.ds(oc * s, s), :], dst_ref=mine,
            send_sem=send_a.at[offset], recv_sem=recv_sem.at[0], device_id=where, device_id_type=MESH,
        )
        copy.start()
        sent.append(copy)
    pltpu.make_async_copy(res.at[pl.ds(column * s, s), :], mine, recv_sem.at[0]).start()

    def flat(ref, first, stride):
        return jnp.concatenate([ref[pl.ds(first + i, n, stride=stride), :] for i in range(s)], axis=1)

    for load in loads[1:4]:
        load.wait()
    eye = (lax.broadcasted_iota(jnp.int32, (n, n), 0) == lax.broadcasted_iota(jnp.int32, (n, n), 1)).astype(jnp.float32)
    inverse = eliminate(gram[...], eye)
    p, q, r = flat(prev, 0, s), flat(prev_img, 0, s), flat(res, 0, s)
    gram_pq = dot_nt(p, q)

    pltpu.make_async_copy(land, land, recv_sem.at[0]).wait()
    field = [
        [
            jnp.concatenate(
                [land[pl.ds(y * n * s + x * lz + z, n, stride=s), :] for y in range(ngy)], axis=1
            )
            for z in range(lz)
        ]
        for x in range(lx)
    ]
    state, image = smooth(field, ngx, ngz)
    for x in range(lx):
        for z in range(lz):
            for y in range(ngy):
                first = y * n * 2 * s + x * lz + z
                cut = slice(y * width, (y + 1) * width)
                done[pl.ds(first, n, stride=2 * s), :] = state[x, z][:, cut]
                done[pl.ds(first + s, n, stride=2 * s), :] = image[x, z][:, cut]
    mine = back.at[pl.ds(column * 2 * s, 2 * s), :]
    for offset, (dx, _, dz) in enumerate(way for way in ways if way[1] == 0):
        oc = lax.rem(gx + dx, ngx) * ngz + lax.rem(gz + dz, ngz)
        copy = pltpu.make_async_remote_copy(
            src_ref=done.at[pl.ds((gy * n + oc) * 2 * s, 2 * s), :], dst_ref=mine,
            send_sem=send_b.at[offset], recv_sem=recv_sem.at[1],
            device_id={"gx": oc // ngz, "gy": gy, "gz": lax.rem(oc, ngz)}, device_id_type=MESH,
        )
        copy.start()
        sent.append(copy)
    pltpu.make_async_copy(done.at[pl.ds(place * 2 * s, 2 * s), :], mine, recv_sem.at[1]).start()
    pltpu.make_async_copy(back, back, recv_sem.at[1]).wait()

    zf, wf = flat(back, 0, 2 * s), flat(back, s, 2 * s)
    sums = dot_nt(zf, jnp.concatenate([r, wf, q], axis=0))
    sums = jnp.concatenate([sums, gram_pq], axis=1)
    keep = pltpu.make_async_copy(back, back_out, local_sem.at[0])
    keep.start()
    half = n // 2
    part[...] = jnp.concatenate([sums[:half], sums[half:]], axis=1)
    mine = parts.at[pl.ds(place * half, half), :]
    for offset in range(1, everyone):
        copy = pltpu.make_async_remote_copy(
            src_ref=part, dst_ref=mine,
            send_sem=send_c.at[offset], recv_sem=recv_sem.at[2], device_id=peer(offset)[1], device_id_type=MESH,
        )
        copy.start()
        sent.append(copy)
    pltpu.make_async_copy(part, mine, recv_sem.at[2]).start()
    pltpu.make_async_copy(parts, parts, recv_sem.at[2]).wait()

    level = [parts[i * half : (i + 1) * half, :] for i in range(everyone)]
    while len(level) > 1:
        level = [sum(level[i + 1 : i + 2], level[i]) for i in range(0, len(level), 2)]
    total = level[0]
    small[:half, :] = total
    small[half:, :] = jnp.concatenate([inverse[:half], inverse[half:], jnp.zeros((half, 6 * n), jnp.float32)], axis=1)
    store = pltpu.make_async_copy(small, small_out, local_sem.at[1])
    store.start()
    for copy in sent:
        copy.wait_send()
    keep.wait()
    store.wait()


def finish(
    sizes, sol_in, res_in, dir_in, img_in, back_in, small_in, sol_out, res_out, dir_out,
    sol, res, prev, prev_img, back, small, outs, local_sem,
):
    ngx, ngy, ngz, n, lx, lz, width = sizes
    s, half = lx * lz, n // 2
    loads = [
        pltpu.make_async_copy(a, b, local_sem.at[i])
        for i, (a, b) in enumerate(
            ((small_in, small), (dir_in, prev), (img_in, prev_img), (back_in, back), (sol_in, sol), (res_in, res))
        )
    ]
    for load in loads:
        load.start()

    def flat(ref, first, stride):
        return jnp.concatenate([ref[pl.ds(first + i, n, stride=stride), :] for i in range(s)], axis=1)

    loads[0].wait()
    total = small[:half, :]
    inverse = small[half:, :]
    inverse = jnp.concatenate([inverse[:, :n], inverse[:, n : 2 * n]], axis=0)
    total = jnp.concatenate([total[:, : 4 * n], total[:, 4 * n :]], axis=0)
    gram_zr, gram_zw, gram_zq, gram_pq = (total[:, i * n : (i + 1) * n] for i in range(4))

    beta = dot(inverse, gram_zr)
    cross = dot(jnp.concatenate([gram_zq, gram_pq], axis=0), beta)
    beta_t = beta.T
    curvature = gram_zw + cross[:n] + cross[:n].T + dot(beta_t, cross[n:])
    for load in loads[1:4]:
        load.wait()
    p, q, zf, wf = flat(prev, 0, s), flat(prev_img, 0, s), flat(back, 0, 2 * s), flat(back, s, 2 * s)
    mixed = dot(beta_t, jnp.concatenate([p, q], axis=1))
    direction = zf + mixed[:, : s * width]
    image_new = wf + mixed[:, s * width :]
    alpha = eliminate(curvature, gram_zr)
    step = dot(alpha.T, jnp.concatenate([direction, image_new], axis=1))
    loads[4].wait()
    loads[5].wait()
    for i in range(s):
        rows = pl.ds(i, n, stride=s)
        cut = slice(i * width, (i + 1) * width)
        outs[2, rows, :] = direction[:, cut]
        outs[0, rows, :] = sol[rows, :] + step[:, cut]
        outs[1, rows, :] = res[rows, :] - step[:, s * width + i * width : s * width + (i + 1) * width]
    stores = [
        pltpu.make_async_copy(outs.at[i], out, local_sem.at[i]) for i, out in enumerate((sol_out, res_out, dir_out))
    ]
    for store in stores:
        store.start()
    for store in stores:
        store.wait()


def whole_body(sizes, solution, residual, direction_prev, image_prev, gram_prev):
    ngx, ngy, ngz, n, lx, lz, width = sizes
    s, everyone = lx * lz, n * ngy
    rows = n * s
    shape = residual.shape
    field = jax.ShapeDtypeStruct((rows, width), jnp.float32)
    anywhere = pl.BlockSpec(memory_space=pl.ANY)
    block = pltpu.VMEM((rows, width), jnp.float32)
    packed = pltpu.VMEM((n, 8 * n), jnp.float32)
    solution, residual, direction_prev, image_prev = (
        a.reshape(rows, width) for a in (solution, residual, direction_prev, image_prev)
    )
    back, small = pl.pallas_call(
        functools.partial(kernel, sizes),
        out_shape=(
            jax.ShapeDtypeStruct((2 * rows, width), jnp.float32),
            jax.ShapeDtypeStruct((n, 8 * n), jnp.float32),
        ),
        in_specs=[anywhere] * 4,
        out_specs=[anywhere] * 2,
        scratch_shapes=[
            block, block, block,
            pltpu.VMEM((n, n), jnp.float32),
            packed,
            pltpu.VMEM((everyone * s, width), jnp.float32),
            pltpu.VMEM((everyone * 2 * s, width), jnp.float32),
            pltpu.VMEM((2 * rows, width), jnp.float32),
            pltpu.VMEM((n // 2, 8 * n), jnp.float32),
            pltpu.VMEM((everyone * (n // 2), 8 * n), jnp.float32),
            pltpu.SemaphoreType.DMA((4,)),
            pltpu.SemaphoreType.DMA((everyone,)),
            pltpu.SemaphoreType.DMA((n,)),
            pltpu.SemaphoreType.DMA((everyone,)),
            pltpu.SemaphoreType.DMA((3,)),
        ],
        compiler_params=pltpu.CompilerParams(collective_id=0, has_side_effects=True),
    )(residual, direction_prev, image_prev, gram_prev)
    outs = pl.pallas_call(
        functools.partial(finish, sizes),
        out_shape=(field, field, field),
        in_specs=[anywhere] * 6,
        out_specs=[anywhere] * 3,
        scratch_shapes=[
            block, block, block, block,
            pltpu.VMEM((2 * rows, width), jnp.float32),
            packed,
            pltpu.VMEM((3, rows, width), jnp.float32),
            pltpu.SemaphoreType.DMA((6,)),
        ],
    )(solution, residual, direction_prev, image_prev, back, small)
    return tuple(a.reshape(shape) for a in outs)


def pick_body(mesh, solution, residual, direction_prev, image_prev, gram_prev):
    ngx, ngy, ngz = (mesh.shape[axis] for axis in ("gx", "gy", "gz"))
    n, lx, lz, width = residual.shape
    fits = n == ngx * ngz and lx % 2 == 0 and lz % 2 == 0 and (lx * lz) % 8 == 0
    fits = fits and width % 128 == 0 and n % 16 == 0
    args = (solution, residual, direction_prev, image_prev, gram_prev)
    if fits:
        return whole_body((ngx, ngy, ngz, n, lx, lz, width), *args)
    return body(*args)


def solution(mesh):
    in_specs = (
        P(None, "gx", "gz", "gy"),
        P(None, "gx", "gz", "gy"),
        P(None, "gx", "gz", "gy"),
        P(None, "gx", "gz", "gy"),
        P(),
    )
    out_specs = (P(None, "gx", "gz", "gy"), P(None, "gx", "gz", "gy"), P(None, "gx", "gz", "gy"))
    return jax.shard_map(functools.partial(pick_body, mesh), mesh=mesh, in_specs=in_specs, out_specs=out_specs, check_vma=False)
```

```python
import functools

import jax
import jax.numpy as jnp
from jax import lax
from jax.experimental import pallas as pl
from jax.experimental.pallas import tpu as pltpu
from jax.sharding import PartitionSpec as P


def with_halo(value, sides, width):
    for axis, dim in sides:
        devices, length = (lax.axis_size(axis), value.shape[dim])
        up = [(i, (i + 1) % devices) for i in range(devices - 1)]
        down = [(j, i) for i, j in up]
        last = lax.slice_in_dim(value, length - width, length, axis=dim)
        first = lax.slice_in_dim(value, 0, width, axis=dim)
        before = lax.ppermute(last, axis, up)
        after = lax.ppermute(first, axis, down)
        value = jnp.concatenate([before, value, after], axis=dim)
    return value


def box_sum(padded):
    total = padded[:, :-2] + padded[:, 1:-1] + padded[:, 2:]
    total = total[:, :, :-2] + total[:, :, 1:-1] + total[:, :, 2:]
    return total[:, :, :, :-2] + total[:, :, :, 1:-1] + total[:, :, :, 2:]


def colors_of(shape):
    first = lax.broadcasted_iota(jnp.int32, shape, 1) % 2
    second = lax.broadcasted_iota(jnp.int32, shape, 2) % 2
    third = lax.broadcasted_iota(jnp.int32, shape, 3) % 2
    return 4 * first + 2 * second + third


def local_gram(left, right):
    return jnp.einsum("kxzy,lxzy->kl", left, right, precision=lax.Precision.HIGHEST)


def combine(field, mixing):
    return jnp.einsum("kxzy,kl->lxzy", field, mixing, precision=lax.Precision.HIGHEST)


def small_dot(left, right):
    return jnp.dot(left, right, precision=lax.Precision.HIGHEST)


def spd_solve(matrix, target):
    order = matrix.shape[0]
    sym = 0.5 * (matrix + matrix.T)
    lower = jnp.zeros_like(sym)
    for col in range(order):
        column = sym[col:, col] - jnp.sum(lower[col:, :col] * lower[col, :col][None, :], axis=1)
        pivot = jnp.sqrt(column[0])
        lower = lower.at[col:, col].set(column / pivot)
    middle = jnp.zeros_like(target)
    for row in range(order):
        value = target[row] - jnp.sum(lower[row, :row][:, None] * middle[:row], axis=0)
        middle = middle.at[row].set(value / lower[row, row])
    answer = jnp.zeros_like(target)
    for row in range(order - 1, -1, -1):
        value = middle[row] - jnp.sum(lower[row + 1 :, row][:, None] * answer[row + 1 :], axis=0)
        answer = answer.at[row].set(value / lower[row, row])
    return answer


def sweep_box(field):
    padded = with_halo(field, (("gx", 1), ("gy", 3), ("gz", 2)), 1)
    return box_sum(padded)


def body(solution, residual, direction_prev, image_prev, gram_prev):
    colors = colors_of(residual.shape)
    smoothed = jnp.where(colors == 0, residual / 26.0, jnp.float32(0.0))
    for shade in list(range(1, 8)) + list(range(6, -1, -1)):
        boxed = sweep_box(smoothed)
        smoothed = jnp.where(colors == shade, (residual + boxed - smoothed) / 26.0, smoothed)
    padded = with_halo(smoothed, (("gx", 1), ("gy", 3), ("gz", 2)), 1)
    image = 27.0 * smoothed - box_sum(padded)
    sums = (
        local_gram(smoothed, residual),
        local_gram(smoothed, image),
        local_gram(smoothed, image_prev),
        local_gram(direction_prev, image),
        local_gram(direction_prev, image_prev),
    )
    gram_zr, gram_zw, gram_zq, gram_pw, gram_pq = lax.psum(
        (sums[0], sums[1], sums[2], sums[3], sums[4]), ("gx", "gy", "gz")
    )
    beta_mix = spd_solve(gram_prev, gram_zr)
    direction = smoothed + combine(direction_prev, beta_mix)
    image_new = image + combine(image_prev, beta_mix)
    curvature = gram_zw + small_dot(gram_zq, beta_mix) + small_dot(beta_mix.T, gram_pw)
    curvature = curvature + small_dot(small_dot(beta_mix.T, gram_pq), beta_mix)
    alpha_step = spd_solve(curvature, gram_zr)
    solution_new = solution + combine(direction, alpha_step)
    residual_new = residual - combine(image_new, alpha_step)
    return (solution_new, residual_new, direction)


MESH = pl.DeviceIdType.MESH
HIGHEST = lax.Precision.HIGHEST


def dot(left, right):
    return jnp.dot(left, right, precision=HIGHEST, preferred_element_type=jnp.float32)


def dot_nt(left, right):
    return lax.dot_general(
        left, right, (((1,), (1,)), ((), ())), precision=HIGHEST, preferred_element_type=jnp.float32
    )


def eliminate(matrix, target):
    matrix = 0.5 * (matrix + matrix.T)
    order = matrix.shape[0]
    rows = lax.broadcasted_iota(jnp.int32, matrix.shape, 0)
    for c in range(order):
        column = jnp.broadcast_to(matrix[:, c : c + 1], matrix.shape)
        scale = 1.0 / column[c : c + 1, :]
        mrow = matrix[c : c + 1, :] * scale
        trow = target[c : c + 1, :] * scale
        here = rows == c
        target = jnp.where(here, trow, target - column * trow)
        if c < order - 1:
            matrix = jnp.where(here, mrow, matrix - column * mrow)
    return target


def smooth(res, ngx, ngz, gy, width):
    lx, lz = len(res), len(res[0])
    count, ny = res[0][0].shape
    row = lax.broadcasted_iota(jnp.int32, (count, ny), 0)
    lane = lax.broadcasted_iota(jnp.int32, (count, ny), 1)
    even = lane % 2 == 0
    edges = {
        "xp": (row < ngz, ngz, 0),
        "xn": (row >= count - ngz, count - ngz, 0),
        "zp": (row % ngz == 0, 1, 0),
        "zn": (row % ngz == ngz - 1, count - 1, 0),
        "yp": (lane == jnp.where(gy == 0, 0, -1), 1, 1),
        "yn": (lane == jnp.where(gy == 0, -1, width - 1), ny - 1, 1),
    }
    zero = jnp.zeros((count, ny), jnp.float32)
    memo = {}

    def moved(value, kind):
        if value is None:
            return None
        key = (kind, id(value))
        if key not in memo:
            edge, amount, axis = edges[kind]
            memo[key] = (value, jnp.where(edge, zero, pltpu.roll(value, amount, axis)))
        return memo[key][1]

    def add(*values):
        total = None
        for value in values:
            if value is not None:
                total = value if total is None else total + value
        return total

    state = {(x, z): None for x in range(lx) for z in range(lz)}

    def z_pair(x, z):
        before = state[x, z - 1] if z > 0 else moved(state[x, lz - 1], "zp")
        after = state[x, z + 1] if z < lz - 1 else moved(state[x, 0], "zn")
        return add(before, after)

    def neighbours(x, z):
        def line(other):
            return add(state[other, z], z_pair(other, z))

        before = line(x - 1) if x > 0 else moved_line(lx - 1, z, "xp")
        after = line(x + 1) if x < lx - 1 else moved_line(0, z, "xn")
        return add(z_pair(x, z), before, after)

    def moved_line(x, z, kind):
        return moved(add(state[x, z], z_pair(x, z)), kind)

    def y_pair(value):
        return moved(value, "yp") + moved(value, "yn")

    third = jnp.float32(1.0 / 26.0)
    plan = [(0, 0, (0, 1)), (0, 1, (0, 1)), (1, 0, (0, 1)), (1, 1, (0, 1, 0)), (1, 0, (1, 0)), (0, 1, (1, 0)), (0, 0, (1, 0))]
    for xp, zp, shades in plan:
        fresh = {}
        for x in range(xp, lx, 2):
            for z in range(zp, lz, 2):
                near = neighbours(x, z)
                base = res[x][z] if near is None else res[x][z] + (near + y_pair(near))
                value = state[x, z]
                for shade in shades:
                    total = base if value is None else base + y_pair(value)
                    chosen = even if shade == 0 else jnp.logical_not(even)
                    value = jnp.where(chosen, total * third, zero if value is None else value)
                fresh[x, z] = value
        state.update(fresh)
    image = {}
    for x in range(lx):
        for z in range(lz):
            box = add(state[x, z], neighbours(x, z))
            image[x, z] = 27.0 * state[x, z] - (box + y_pair(box))
    return state, image


def kernel(
    sizes, res_in, dir_in, img_in, gram_in, back_out, small_out,
    res, prev, prev_img, gram, small, land, strip, halo, done, back, part, parts,
    local_sem, send_a, send_b, send_c, recv_sem,
):
    ngx, ngy, ngz, n, lx, lz, width = sizes
    s = lx * lz
    gx, gy, gz = lax.axis_index("gx"), lax.axis_index("gy"), lax.axis_index("gz")
    column = gx * ngz + gz
    place = gy * n + column
    everyone = n * ngy

    loads = [
        pltpu.make_async_copy(a, b, local_sem.at[i])
        for i, (a, b) in enumerate(((res_in, res), (gram_in, gram), (dir_in, prev), (img_in, prev_img)))
    ]
    for load in loads:
        load.start()

    ways = sorted(
        ((dx, dy, dz) for dx in range(ngx) for dy in range(ngy) for dz in range(ngz)),
        key=lambda way: (-min(way[2], ngz - way[2]), -min(way[0], ngx - way[0]), -way[1]),
    )[:-1]

    def peer(offset):
        dx, dy, dz = ways[offset - 1]
        ox, oy, oz = lax.rem(gx + dx, ngx), lax.rem(gy + dy, ngy), lax.rem(gz + dz, ngz)
        return ox * ngz + oz, {"gx": ox, "gy": oy, "gz": oz}

    barrier = pltpu.get_barrier_semaphore()
    for offset in range(1, everyone):
        pl.semaphore_signal(barrier, inc=1, device_id=peer(offset)[1], device_id_type=MESH)
    loads[0].wait()
    depth = width // s
    lanes = lax.broadcasted_iota(jnp.int32, (n, width), 1)
    packed = jnp.zeros((n, width), jnp.float32)
    for i in range(s):
        line = res[pl.ds(i, n, stride=s), :]
        line = pltpu.roll(line, lax.rem(i * depth + jnp.where(gy == 0, depth, 0), width), 1)
        packed = jnp.where(lanes // depth == i, line, packed)
    for i in range(n):
        strip[i] = packed[i : i + 1, :]
    pl.semaphore_wait(barrier, everyone - 1)

    sent = []
    mine = land.at[pl.ds(column * s, s), :]
    for offset in range(1, everyone):
        oc, where = peer(offset)
        near = ways[offset - 1][1] == 0
        copy = pltpu.make_async_remote_copy(
            src_ref=res.at[pl.ds(oc * s, s), :] if near else strip.at[oc],
            dst_ref=mine if near else halo.at[column],
            send_sem=send_a.at[offset], recv_sem=recv_sem.at[0 if near else 3],
            device_id=where, device_id_type=MESH,
        )
        copy.start()
        sent.append(copy)
    pltpu.make_async_copy(res.at[pl.ds(column * s, s), :], mine, recv_sem.at[0]).start()

    def flat(ref, first, stride):
        return jnp.concatenate([ref[pl.ds(first + i, n, stride=stride), :] for i in range(s)], axis=1)

    for load in loads[1:4]:
        load.wait()
    eye = (lax.broadcasted_iota(jnp.int32, (n, n), 0) == lax.broadcasted_iota(jnp.int32, (n, n), 1)).astype(jnp.float32)
    inverse = eliminate(gram[...], eye)
    p, q, r = flat(prev, 0, s), flat(prev_img, 0, s), flat(res, 0, s)
    gram_pq = dot_nt(p, q)

    pltpu.make_async_copy(land, land, recv_sem.at[0]).wait()
    pltpu.make_async_copy(halo, halo, recv_sem.at[3]).wait()
    rows = jnp.concatenate([halo[i] for i in range(n)], axis=0)
    outside = jnp.where(gy == 0, 0, s - 1)

    def extended(i):
        shift = lax.rem((2 * s - i + outside) * depth, width)
        beside = jnp.where(lanes // depth == outside, pltpu.roll(rows, shift, 1), 0.0)
        return jnp.concatenate([land[pl.ds(i, n, stride=s), :], beside], axis=1)

    field = [[extended(x * lz + z) for z in range(lz)] for x in range(lx)]
    state, image = smooth(field, ngx, ngz, gy, width)
    for x in range(lx):
        for z in range(lz):
            first = x * lz + z
            done[pl.ds(first, n, stride=2 * s), :] = state[x, z][:, :width]
            done[pl.ds(first + s, n, stride=2 * s), :] = image[x, z][:, :width]
    mine = back.at[pl.ds(column * 2 * s, 2 * s), :]
    for offset, (dx, _, dz) in enumerate(way for way in ways if way[1] == 0):
        oc = lax.rem(gx + dx, ngx) * ngz + lax.rem(gz + dz, ngz)
        copy = pltpu.make_async_remote_copy(
            src_ref=done.at[pl.ds(oc * 2 * s, 2 * s), :], dst_ref=mine,
            send_sem=send_b.at[offset], recv_sem=recv_sem.at[1],
            device_id={"gx": oc // ngz, "gy": gy, "gz": lax.rem(oc, ngz)}, device_id_type=MESH,
        )
        copy.start()
        sent.append(copy)
    pltpu.make_async_copy(done.at[pl.ds(column * 2 * s, 2 * s), :], mine, recv_sem.at[1]).start()
    pltpu.make_async_copy(back, back, recv_sem.at[1]).wait()

    zf, wf = flat(back, 0, 2 * s), flat(back, s, 2 * s)
    sums = dot_nt(zf, jnp.concatenate([r, wf, q], axis=0))
    sums = jnp.concatenate([sums, gram_pq], axis=1)
    keep = pltpu.make_async_copy(back, back_out, local_sem.at[0])
    keep.start()
    half = n // 2
    part[...] = jnp.concatenate([sums[:half], sums[half:]], axis=1)
    mine = parts.at[pl.ds(place * half, half), :]
    for offset in range(1, everyone):
        copy = pltpu.make_async_remote_copy(
            src_ref=part, dst_ref=mine,
            send_sem=send_c.at[offset], recv_sem=recv_sem.at[2], device_id=peer(offset)[1], device_id_type=MESH,
        )
        copy.start()
        sent.append(copy)
    pltpu.make_async_copy(part, mine, recv_sem.at[2]).start()
    pltpu.make_async_copy(parts, parts, recv_sem.at[2]).wait()

    level = [parts[i * half : (i + 1) * half, :] for i in range(everyone)]
    while len(level) > 1:
        level = [sum(level[i + 1 : i + 2], level[i]) for i in range(0, len(level), 2)]
    total = level[0]
    small[:half, :] = total
    small[half:, :] = jnp.concatenate([inverse[:half], inverse[half:], jnp.zeros((half, 6 * n), jnp.float32)], axis=1)
    store = pltpu.make_async_copy(small, small_out, local_sem.at[1])
    store.start()
    for copy in sent:
        copy.wait_send()
    keep.wait()
    store.wait()


def finish(
    sizes, sol_in, res_in, dir_in, img_in, back_in, small_in, sol_out, res_out, dir_out,
    sol, res, prev, prev_img, back, small, outs, local_sem,
):
    ngx, ngy, ngz, n, lx, lz, width = sizes
    s, half = lx * lz, n // 2
    loads = [
        pltpu.make_async_copy(a, b, local_sem.at[i])
        for i, (a, b) in enumerate(
            ((small_in, small), (dir_in, prev), (img_in, prev_img), (back_in, back), (sol_in, sol), (res_in, res))
        )
    ]
    for load in loads:
        load.start()

    def flat(ref, first, stride):
        return jnp.concatenate([ref[pl.ds(first + i, n, stride=stride), :] for i in range(s)], axis=1)

    loads[0].wait()
    total = small[:half, :]
    inverse = small[half:, :]
    inverse = jnp.concatenate([inverse[:, :n], inverse[:, n : 2 * n]], axis=0)
    total = jnp.concatenate([total[:, : 4 * n], total[:, 4 * n :]], axis=0)
    gram_zr, gram_zw, gram_zq, gram_pq = (total[:, i * n : (i + 1) * n] for i in range(4))

    beta = dot(inverse, gram_zr)
    cross = dot(jnp.concatenate([gram_zq, gram_pq], axis=0), beta)
    beta_t = beta.T
    curvature = gram_zw + cross[:n] + cross[:n].T + dot(beta_t, cross[n:])
    for load in loads[1:4]:
        load.wait()
    p, q, zf, wf = flat(prev, 0, s), flat(prev_img, 0, s), flat(back, 0, 2 * s), flat(back, s, 2 * s)
    mixed = dot(beta_t, jnp.concatenate([p, q], axis=1))
    direction = zf + mixed[:, : s * width]
    image_new = wf + mixed[:, s * width :]
    alpha = eliminate(curvature, gram_zr)
    step = dot(alpha.T, jnp.concatenate([direction, image_new], axis=1))
    loads[4].wait()
    loads[5].wait()
    for i in range(s):
        rows = pl.ds(i, n, stride=s)
        cut = slice(i * width, (i + 1) * width)
        outs[2, rows, :] = direction[:, cut]
        outs[0, rows, :] = sol[rows, :] + step[:, cut]
        outs[1, rows, :] = res[rows, :] - step[:, s * width + i * width : s * width + (i + 1) * width]
    stores = [
        pltpu.make_async_copy(outs.at[i], out, local_sem.at[i]) for i, out in enumerate((sol_out, res_out, dir_out))
    ]
    for store in stores:
        store.start()
    for store in stores:
        store.wait()


def whole_body(sizes, solution, residual, direction_prev, image_prev, gram_prev):
    ngx, ngy, ngz, n, lx, lz, width = sizes
    s, everyone = lx * lz, n * ngy
    rows = n * s
    shape = residual.shape
    field = jax.ShapeDtypeStruct((rows, width), jnp.float32)
    anywhere = pl.BlockSpec(memory_space=pl.ANY)
    block = pltpu.VMEM((rows, width), jnp.float32)
    packed = pltpu.VMEM((n, 8 * n), jnp.float32)
    solution, residual, direction_prev, image_prev = (
        a.reshape(rows, width) for a in (solution, residual, direction_prev, image_prev)
    )
    back, small = pl.pallas_call(
        functools.partial(kernel, sizes),
        out_shape=(
            jax.ShapeDtypeStruct((2 * rows, width), jnp.float32),
            jax.ShapeDtypeStruct((n, 8 * n), jnp.float32),
        ),
        in_specs=[anywhere] * 4,
        out_specs=[anywhere] * 2,
        scratch_shapes=[
            block, block, block,
            pltpu.VMEM((n, n), jnp.float32),
            packed,
            pltpu.VMEM((rows, width), jnp.float32),
            pltpu.VMEM((n, 1, width), jnp.float32),
            pltpu.VMEM((n, 1, width), jnp.float32),
            pltpu.VMEM((2 * rows, width), jnp.float32),
            pltpu.VMEM((2 * rows, width), jnp.float32),
            pltpu.VMEM((n // 2, 8 * n), jnp.float32),
            pltpu.VMEM((everyone * (n // 2), 8 * n), jnp.float32),
            pltpu.SemaphoreType.DMA((4,)),
            pltpu.SemaphoreType.DMA((everyone,)),
            pltpu.SemaphoreType.DMA((n,)),
            pltpu.SemaphoreType.DMA((everyone,)),
            pltpu.SemaphoreType.DMA((4,)),
        ],
        compiler_params=pltpu.CompilerParams(collective_id=0, has_side_effects=True),
    )(residual, direction_prev, image_prev, gram_prev)
    outs = pl.pallas_call(
        functools.partial(finish, sizes),
        out_shape=(field, field, field),
        in_specs=[anywhere] * 6,
        out_specs=[anywhere] * 3,
        scratch_shapes=[
            block, block, block, block,
            pltpu.VMEM((2 * rows, width), jnp.float32),
            packed,
            pltpu.VMEM((3, rows, width), jnp.float32),
            pltpu.SemaphoreType.DMA((6,)),
        ],
    )(solution, residual, direction_prev, image_prev, back, small)
    return tuple(a.reshape(shape) for a in outs)


def pick_body(mesh, solution, residual, direction_prev, image_prev, gram_prev):
    ngx, ngy, ngz = (mesh.shape[axis] for axis in ("gx", "gy", "gz"))
    n, lx, lz, width = residual.shape
    fits = n == ngx * ngz and lx % 2 == 0 and lz % 2 == 0 and (lx * lz) % 8 == 0
    fits = fits and width % 128 == 0 and n % 16 == 0 and ngy == 2 and width % (lx * lz) == 0 and width // (lx * lz) >= 15
    args = (solution, residual, direction_prev, image_prev, gram_prev)
    if fits:
        return whole_body((ngx, ngy, ngz, n, lx, lz, width), *args)
    return body(*args)


def solution(mesh):
    in_specs = (
        P(None, "gx", "gz", "gy"),
        P(None, "gx", "gz", "gy"),
        P(None, "gx", "gz", "gy"),
        P(None, "gx", "gz", "gy"),
        P(),
    )
    out_specs = (P(None, "gx", "gz", "gy"), P(None, "gx", "gz", "gy"), P(None, "gx", "gz", "gy"))
    return jax.shard_map(functools.partial(pick_body, mesh), mesh=mesh, in_specs=in_specs, out_specs=out_specs, check_vma=False)
```

```python
import functools

import jax
import jax.numpy as jnp
from jax import lax
from jax.experimental import pallas as pl
from jax.experimental.pallas import tpu as pltpu
from jax.sharding import PartitionSpec as P


def with_halo(value, sides, width):
    for axis, dim in sides:
        devices, length = (lax.axis_size(axis), value.shape[dim])
        up = [(i, (i + 1) % devices) for i in range(devices - 1)]
        down = [(j, i) for i, j in up]
        last = lax.slice_in_dim(value, length - width, length, axis=dim)
        first = lax.slice_in_dim(value, 0, width, axis=dim)
        before = lax.ppermute(last, axis, up)
        after = lax.ppermute(first, axis, down)
        value = jnp.concatenate([before, value, after], axis=dim)
    return value


def box_sum(padded):
    total = padded[:, :-2] + padded[:, 1:-1] + padded[:, 2:]
    total = total[:, :, :-2] + total[:, :, 1:-1] + total[:, :, 2:]
    return total[:, :, :, :-2] + total[:, :, :, 1:-1] + total[:, :, :, 2:]


def colors_of(shape):
    first = lax.broadcasted_iota(jnp.int32, shape, 1) % 2
    second = lax.broadcasted_iota(jnp.int32, shape, 2) % 2
    third = lax.broadcasted_iota(jnp.int32, shape, 3) % 2
    return 4 * first + 2 * second + third


def local_gram(left, right):
    return jnp.einsum("kxzy,lxzy->kl", left, right, precision=lax.Precision.HIGHEST)


def combine(field, mixing):
    return jnp.einsum("kxzy,kl->lxzy", field, mixing, precision=lax.Precision.HIGHEST)


def small_dot(left, right):
    return jnp.dot(left, right, precision=lax.Precision.HIGHEST)


def spd_solve(matrix, target):
    order = matrix.shape[0]
    sym = 0.5 * (matrix + matrix.T)
    lower = jnp.zeros_like(sym)
    for col in range(order):
        column = sym[col:, col] - jnp.sum(lower[col:, :col] * lower[col, :col][None, :], axis=1)
        pivot = jnp.sqrt(column[0])
        lower = lower.at[col:, col].set(column / pivot)
    middle = jnp.zeros_like(target)
    for row in range(order):
        value = target[row] - jnp.sum(lower[row, :row][:, None] * middle[:row], axis=0)
        middle = middle.at[row].set(value / lower[row, row])
    answer = jnp.zeros_like(target)
    for row in range(order - 1, -1, -1):
        value = middle[row] - jnp.sum(lower[row + 1 :, row][:, None] * answer[row + 1 :], axis=0)
        answer = answer.at[row].set(value / lower[row, row])
    return answer


def sweep_box(field):
    padded = with_halo(field, (("gx", 1), ("gy", 3), ("gz", 2)), 1)
    return box_sum(padded)


def body(solution, residual, direction_prev, image_prev, gram_prev):
    colors = colors_of(residual.shape)
    smoothed = jnp.where(colors == 0, residual / 26.0, jnp.float32(0.0))
    for shade in list(range(1, 8)) + list(range(6, -1, -1)):
        boxed = sweep_box(smoothed)
        smoothed = jnp.where(colors == shade, (residual + boxed - smoothed) / 26.0, smoothed)
    padded = with_halo(smoothed, (("gx", 1), ("gy", 3), ("gz", 2)), 1)
    image = 27.0 * smoothed - box_sum(padded)
    sums = (
        local_gram(smoothed, residual),
        local_gram(smoothed, image),
        local_gram(smoothed, image_prev),
        local_gram(direction_prev, image),
        local_gram(direction_prev, image_prev),
    )
    gram_zr, gram_zw, gram_zq, gram_pw, gram_pq = lax.psum(
        (sums[0], sums[1], sums[2], sums[3], sums[4]), ("gx", "gy", "gz")
    )
    beta_mix = spd_solve(gram_prev, gram_zr)
    direction = smoothed + combine(direction_prev, beta_mix)
    image_new = image + combine(image_prev, beta_mix)
    curvature = gram_zw + small_dot(gram_zq, beta_mix) + small_dot(beta_mix.T, gram_pw)
    curvature = curvature + small_dot(small_dot(beta_mix.T, gram_pq), beta_mix)
    alpha_step = spd_solve(curvature, gram_zr)
    solution_new = solution + combine(direction, alpha_step)
    residual_new = residual - combine(image_new, alpha_step)
    return (solution_new, residual_new, direction)


MESH = pl.DeviceIdType.MESH
HIGHEST = lax.Precision.HIGHEST


def dot(left, right):
    return jnp.dot(left, right, precision=HIGHEST, preferred_element_type=jnp.float32)


def dot_nt(left, right):
    return lax.dot_general(
        left, right, (((1,), (1,)), ((), ())), precision=HIGHEST, preferred_element_type=jnp.float32
    )


def eliminate(matrix, target):
    order = matrix.shape[0]
    both = jnp.concatenate([0.5 * (matrix + matrix.T), target], axis=1)
    rows = lax.broadcasted_iota(jnp.int32, both.shape, 0)
    for c in range(order):
        column = jnp.broadcast_to(both[:, c : c + 1], both.shape)
        line = both[c : c + 1, :] / column[c : c + 1, :]
        both = jnp.where(rows == c, line, both - column * line)
    return both[:, order:]


def smooth(res, ngx, ngz, gy, width):
    lx, lz = len(res), len(res[0])
    count, ny = res[0][0].shape
    row = lax.broadcasted_iota(jnp.int32, (count, ny), 0)
    lane = lax.broadcasted_iota(jnp.int32, (count, ny), 1)
    even = lane % 2 == 0
    edges = {
        "xp": (row < ngz, ngz, 0),
        "xn": (row >= count - ngz, count - ngz, 0),
        "zp": (row % ngz == 0, 1, 0),
        "zn": (row % ngz == ngz - 1, count - 1, 0),
        "yp": (lane == jnp.where(gy == 0, 0, -1), 1, 1),
        "yn": (lane == jnp.where(gy == 0, -1, width - 1), ny - 1, 1),
    }
    zero = jnp.zeros((count, ny), jnp.float32)
    memo = {}

    def moved(value, kind):
        if value is None:
            return None
        key = (kind, id(value))
        if key not in memo:
            edge, amount, axis = edges[kind]
            memo[key] = (value, jnp.where(edge, zero, pltpu.roll(value, amount, axis)))
        return memo[key][1]

    def add(*values):
        total = None
        for value in values:
            if value is not None:
                total = value if total is None else total + value
        return total

    state = {(x, z): None for x in range(lx) for z in range(lz)}

    def z_pair(x, z):
        before = state[x, z - 1] if z > 0 else moved(state[x, lz - 1], "zp")
        after = state[x, z + 1] if z < lz - 1 else moved(state[x, 0], "zn")
        return add(before, after)

    def neighbours(x, z):
        def line(other):
            return add(state[other, z], z_pair(other, z))

        before = line(x - 1) if x > 0 else moved_line(lx - 1, z, "xp")
        after = line(x + 1) if x < lx - 1 else moved_line(0, z, "xn")
        return add(z_pair(x, z), before, after)

    def moved_line(x, z, kind):
        return moved(add(state[x, z], z_pair(x, z)), kind)

    def y_pair(value):
        return moved(value, "yp") + moved(value, "yn")

    third = jnp.float32(1.0 / 26.0)
    plan = [(0, 0, (0, 1)), (0, 1, (0, 1)), (1, 0, (0, 1)), (1, 1, (0, 1, 0)), (1, 0, (1, 0)), (0, 1, (1, 0)), (0, 0, (1, 0))]
    for xp, zp, shades in plan:
        fresh = {}
        for x in range(xp, lx, 2):
            for z in range(zp, lz, 2):
                near = neighbours(x, z)
                base = res[x][z] if near is None else res[x][z] + (near + y_pair(near))
                value = state[x, z]
                for shade in shades:
                    total = base if value is None else base + y_pair(value)
                    chosen = even if shade == 0 else jnp.logical_not(even)
                    value = jnp.where(chosen, total * third, zero if value is None else value)
                fresh[x, z] = value
        state.update(fresh)
    image = {}
    for x in range(lx):
        for z in range(lz):
            box = add(state[x, z], neighbours(x, z))
            image[x, z] = 27.0 * state[x, z] - (box + y_pair(box))
    return state, image


def kernel(
    sizes, res_in, dir_in, img_in, gram_in, back_out, small_out,
    res, prev, prev_img, gram, small, land, strip, halo, done, back, part, parts,
    local_sem, send_a, send_b, send_c, recv_sem,
):
    ngx, ngy, ngz, n, lx, lz, width = sizes
    s = lx * lz
    gx, gy, gz = lax.axis_index("gx"), lax.axis_index("gy"), lax.axis_index("gz")
    column = gx * ngz + gz
    place = gy * n + column
    everyone = n * ngy

    loads = [
        pltpu.make_async_copy(a, b, local_sem.at[i])
        for i, (a, b) in enumerate(((res_in, res), (gram_in, gram), (dir_in, prev), (img_in, prev_img)))
    ]
    for load in loads:
        load.start()

    ways = sorted(
        ((dx, dy, dz) for dx in range(ngx) for dy in range(ngy) for dz in range(ngz)),
        key=lambda way: (-min(way[2], ngz - way[2]), -min(way[0], ngx - way[0]), -way[1]),
    )[:-1]

    def peer(offset):
        dx, dy, dz = ways[offset - 1]
        ox, oy, oz = lax.rem(gx + dx, ngx), lax.rem(gy + dy, ngy), lax.rem(gz + dz, ngz)
        return ox * ngz + oz, {"gx": ox, "gy": oy, "gz": oz}

    barrier = pltpu.get_barrier_semaphore()
    for offset in range(1, everyone):
        pl.semaphore_signal(barrier, inc=1, device_id=peer(offset)[1], device_id_type=MESH)
    loads[0].wait()
    depth = width // s
    lanes = lax.broadcasted_iota(jnp.int32, (n, width), 1)
    packed = jnp.zeros((n, width), jnp.float32)
    for i in range(s):
        line = res[pl.ds(i, n, stride=s), :]
        line = pltpu.roll(line, lax.rem(i * depth + jnp.where(gy == 0, depth, 0), width), 1)
        packed = jnp.where(lanes // depth == i, line, packed)
    for i in range(n):
        strip[i] = packed[i : i + 1, :]
    pl.semaphore_wait(barrier, everyone - 1)

    sent = []
    mine = land.at[pl.ds(column * s, s), :]
    for offset in range(1, everyone):
        oc, where = peer(offset)
        near = ways[offset - 1][1] == 0
        copy = pltpu.make_async_remote_copy(
            src_ref=res.at[pl.ds(oc * s, s), :] if near else strip.at[oc],
            dst_ref=mine if near else halo.at[column],
            send_sem=send_a.at[offset], recv_sem=recv_sem.at[0 if near else 3],
            device_id=where, device_id_type=MESH,
        )
        copy.start()
        sent.append(copy)
    pltpu.make_async_copy(res.at[pl.ds(column * s, s), :], mine, recv_sem.at[0]).start()

    def flat(ref, first, stride):
        return jnp.concatenate([ref[pl.ds(first + i, n, stride=stride), :] for i in range(s)], axis=1)

    for load in loads[1:4]:
        load.wait()
    eye = (lax.broadcasted_iota(jnp.int32, (n, n), 0) == lax.broadcasted_iota(jnp.int32, (n, n), 1)).astype(jnp.float32)
    inverse = eliminate(gram[...], eye)
    p, q, r = flat(prev, 0, s), flat(prev_img, 0, s), flat(res, 0, s)
    gram_pq = dot_nt(p, q)

    pltpu.make_async_copy(land, land, recv_sem.at[0]).wait()
    pltpu.make_async_copy(halo, halo, recv_sem.at[3]).wait()
    rows = jnp.concatenate([halo[i] for i in range(n)], axis=0)
    outside = jnp.where(gy == 0, 0, s - 1)

    def extended(i):
        shift = lax.rem((2 * s - i + outside) * depth, width)
        beside = jnp.where(lanes // depth == outside, pltpu.roll(rows, shift, 1), 0.0)
        return jnp.concatenate([land[pl.ds(i, n, stride=s), :], beside], axis=1)

    field = [[extended(x * lz + z) for z in range(lz)] for x in range(lx)]
    state, image = smooth(field, ngx, ngz, gy, width)
    for x in range(lx):
        for z in range(lz):
            first = x * lz + z
            done[pl.ds(first, n, stride=2 * s), :] = state[x, z][:, :width]
            done[pl.ds(first + s, n, stride=2 * s), :] = image[x, z][:, :width]
    mine = back.at[pl.ds(column * 2 * s, 2 * s), :]
    for offset, (dx, _, dz) in enumerate(way for way in ways if way[1] == 0):
        oc = lax.rem(gx + dx, ngx) * ngz + lax.rem(gz + dz, ngz)
        copy = pltpu.make_async_remote_copy(
            src_ref=done.at[pl.ds(oc * 2 * s, 2 * s), :], dst_ref=mine,
            send_sem=send_b.at[offset], recv_sem=recv_sem.at[1],
            device_id={"gx": oc // ngz, "gy": gy, "gz": lax.rem(oc, ngz)}, device_id_type=MESH,
        )
        copy.start()
        sent.append(copy)
    pltpu.make_async_copy(done.at[pl.ds(column * 2 * s, 2 * s), :], mine, recv_sem.at[1]).start()
    pltpu.make_async_copy(back, back, recv_sem.at[1]).wait()

    zf, wf = flat(back, 0, 2 * s), flat(back, s, 2 * s)
    sums = dot_nt(zf, jnp.concatenate([r, wf, q], axis=0))
    sums = jnp.concatenate([sums, gram_pq], axis=1)
    keep = pltpu.make_async_copy(back, back_out, local_sem.at[0])
    keep.start()
    half = n // 2
    part[...] = jnp.concatenate([sums[:half], sums[half:]], axis=1)
    mine = parts.at[pl.ds(place * half, half), :]
    for offset in range(1, everyone):
        copy = pltpu.make_async_remote_copy(
            src_ref=part, dst_ref=mine,
            send_sem=send_c.at[offset], recv_sem=recv_sem.at[2], device_id=peer(offset)[1], device_id_type=MESH,
        )
        copy.start()
        sent.append(copy)
    pltpu.make_async_copy(part, mine, recv_sem.at[2]).start()
    pltpu.make_async_copy(parts, parts, recv_sem.at[2]).wait()

    level = [parts[i * half : (i + 1) * half, :] for i in range(everyone)]
    while len(level) > 1:
        level = [sum(level[i + 1 : i + 2], level[i]) for i in range(0, len(level), 2)]
    total = level[0]
    small[:half, :] = total
    small[half:, :] = jnp.concatenate([inverse[:half], inverse[half:], jnp.zeros((half, 6 * n), jnp.float32)], axis=1)
    store = pltpu.make_async_copy(small, small_out, local_sem.at[1])
    store.start()
    for copy in sent:
        copy.wait_send()
    keep.wait()
    store.wait()


def finish(
    sizes, sol_in, res_in, dir_in, img_in, back_in, small_in, sol_out, res_out, dir_out,
    sol, res, prev, prev_img, back, small, outs, local_sem,
):
    ngx, ngy, ngz, n, lx, lz, width = sizes
    s, half = lx * lz, n // 2
    loads = [
        pltpu.make_async_copy(a, b, local_sem.at[i])
        for i, (a, b) in enumerate(
            ((small_in, small), (dir_in, prev), (img_in, prev_img), (back_in, back), (sol_in, sol), (res_in, res))
        )
    ]
    for load in loads:
        load.start()

    def flat(ref, first, stride):
        return jnp.concatenate([ref[pl.ds(first + i, n, stride=stride), :] for i in range(s)], axis=1)

    loads[0].wait()
    total = small[:half, :]
    inverse = small[half:, :]
    inverse = jnp.concatenate([inverse[:, :n], inverse[:, n : 2 * n]], axis=0)
    total = jnp.concatenate([total[:, : 4 * n], total[:, 4 * n :]], axis=0)
    gram_zr, gram_zw, gram_zq, gram_pq = (total[:, i * n : (i + 1) * n] for i in range(4))

    beta = dot(inverse, gram_zr)
    cross = dot(jnp.concatenate([gram_zq, gram_pq], axis=0), beta)
    beta_t = beta.T
    curvature = gram_zw + cross[:n] + cross[:n].T + dot(beta_t, cross[n:])
    for load in loads[1:4]:
        load.wait()
    p, q, zf, wf = flat(prev, 0, s), flat(prev_img, 0, s), flat(back, 0, 2 * s), flat(back, s, 2 * s)
    mixed = dot(beta_t, jnp.concatenate([p, q], axis=1))
    direction = zf + mixed[:, : s * width]
    image_new = wf + mixed[:, s * width :]
    alpha = eliminate(curvature, gram_zr)
    step = dot(alpha.T, jnp.concatenate([direction, image_new], axis=1))
    loads[4].wait()
    loads[5].wait()
    for i in range(s):
        rows = pl.ds(i, n, stride=s)
        cut = slice(i * width, (i + 1) * width)
        outs[2, rows, :] = direction[:, cut]
        outs[0, rows, :] = sol[rows, :] + step[:, cut]
        outs[1, rows, :] = res[rows, :] - step[:, s * width + i * width : s * width + (i + 1) * width]
    stores = [
        pltpu.make_async_copy(outs.at[i], out, local_sem.at[i]) for i, out in enumerate((sol_out, res_out, dir_out))
    ]
    for store in stores:
        store.start()
    for store in stores:
        store.wait()


def whole_body(sizes, solution, residual, direction_prev, image_prev, gram_prev):
    ngx, ngy, ngz, n, lx, lz, width = sizes
    s, everyone = lx * lz, n * ngy
    rows = n * s
    shape = residual.shape
    field = jax.ShapeDtypeStruct((rows, width), jnp.float32)
    anywhere = pl.BlockSpec(memory_space=pl.ANY)
    block = pltpu.VMEM((rows, width), jnp.float32)
    packed = pltpu.VMEM((n, 8 * n), jnp.float32)
    solution, residual, direction_prev, image_prev = (
        a.reshape(rows, width) for a in (solution, residual, direction_prev, image_prev)
    )
    back, small = pl.pallas_call(
        functools.partial(kernel, sizes),
        out_shape=(
            jax.ShapeDtypeStruct((2 * rows, width), jnp.float32),
            jax.ShapeDtypeStruct((n, 8 * n), jnp.float32),
        ),
        in_specs=[anywhere] * 4,
        out_specs=[anywhere] * 2,
        scratch_shapes=[
            block, block, block,
            pltpu.VMEM((n, n), jnp.float32),
            packed,
            pltpu.VMEM((rows, width), jnp.float32),
            pltpu.VMEM((n, 1, width), jnp.float32),
            pltpu.VMEM((n, 1, width), jnp.float32),
            pltpu.VMEM((2 * rows, width), jnp.float32),
            pltpu.VMEM((2 * rows, width), jnp.float32),
            pltpu.VMEM((n // 2, 8 * n), jnp.float32),
            pltpu.VMEM((everyone * (n // 2), 8 * n), jnp.float32),
            pltpu.SemaphoreType.DMA((4,)),
            pltpu.SemaphoreType.DMA((everyone,)),
            pltpu.SemaphoreType.DMA((n,)),
            pltpu.SemaphoreType.DMA((everyone,)),
            pltpu.SemaphoreType.DMA((4,)),
        ],
        compiler_params=pltpu.CompilerParams(collective_id=0, has_side_effects=True),
    )(residual, direction_prev, image_prev, gram_prev)
    outs = pl.pallas_call(
        functools.partial(finish, sizes),
        out_shape=(field, field, field),
        in_specs=[anywhere] * 6,
        out_specs=[anywhere] * 3,
        scratch_shapes=[
            block, block, block, block,
            pltpu.VMEM((2 * rows, width), jnp.float32),
            packed,
            pltpu.VMEM((3, rows, width), jnp.float32),
            pltpu.SemaphoreType.DMA((6,)),
        ],
    )(solution, residual, direction_prev, image_prev, back, small)
    return tuple(a.reshape(shape) for a in outs)


def pick_body(mesh, solution, residual, direction_prev, image_prev, gram_prev):
    ngx, ngy, ngz = (mesh.shape[axis] for axis in ("gx", "gy", "gz"))
    n, lx, lz, width = residual.shape
    fits = n == ngx * ngz and lx % 2 == 0 and lz % 2 == 0 and (lx * lz) % 8 == 0
    fits = fits and width % 128 == 0 and n % 16 == 0 and ngy == 2 and width % (lx * lz) == 0 and width // (lx * lz) >= 15
    args = (solution, residual, direction_prev, image_prev, gram_prev)
    if fits:
        return whole_body((ngx, ngy, ngz, n, lx, lz, width), *args)
    return body(*args)


def solution(mesh):
    in_specs = (
        P(None, "gx", "gz", "gy"),
        P(None, "gx", "gz", "gy"),
        P(None, "gx", "gz", "gy"),
        P(None, "gx", "gz", "gy"),
        P(),
    )
    out_specs = (P(None, "gx", "gz", "gy"), P(None, "gx", "gz", "gy"), P(None, "gx", "gz", "gy"))
    return jax.shard_map(functools.partial(pick_body, mesh), mesh=mesh, in_specs=in_specs, out_specs=out_specs, check_vma=False)
```
